8 devices in a mesh: data: 1 (over z), pp: 2 (over y), ep: 4 (over x, core).
Axes of the slice: x: 2, y: 2, z: 1, core: 2. Of those that a mesh axis runs over, the one named last changes fastest.
Arguments:
- O: bfloat16 [2, 6, 128, 64, 4096], P(('data', 'pp'), None, 'ep')
- idx: int32 [2, 6, 4, 128, 8], P(('data', 'pp'), None, 'ep')
- slot: int32 [2, 6, 4, 128, 8], P(('data', 'pp'), None, 'ep')
- g: float32 [2, 6, 4, 128, 8], P(('data', 'pp'), None, 'ep')
- H: bfloat16 [2, 6, 4, 128, 4096], P(('data', 'pp'), None, 'ep')
- w: float32 [2, 4096], P('pp')
- Wq: bfloat16 [2, 4096, 64, 128], P('pp')
- Wk: bfloat16 [2, 4096, 64, 128], P('pp')
- Wv: bfloat16 [2, 4096, 64, 128], P('pp')
- Wo: bfloat16 [2, 64, 128, 4096], P('pp')
Outputs:
- output: bfloat16 [2, 6, 4, 128, 4096], P(('data', 'pp'), None, 'ep')
All inputs are finite; a program needn't handle non-finite values.
Results may differ from the reference program's by a relative error of at most 0.0127664.
Values are sent between devices in bfloat16 or wider.
A program may use at most 1.5 GiB of HBM per device.

```python
import math
import jax
import jax.numpy as jnp
from jax import lax

PP = 2
EP = 4
M = 6
SEQ_DEV = 1
L = 128
D = 4096
HEADS = 64
HEAD_DIM = 128
EXPERTS = 128
TOP = 8
CG = 16

EPS = 1e-6
SEQS = EP * SEQ_DEV
TD = SEQ_DEV * L
T = EP * TD
C = EP * CG
QKV = HEADS * HEAD_DIM


def ranks(e, pr):
    n = e.shape[0]
    order = jnp.argsort(e * n + pr)
    se = e[order]
    start = jnp.searchsorted(se, se, side='left').astype(jnp.int32)
    r = jnp.arange(n, dtype=jnp.int32) - start
    return jnp.zeros((n,), jnp.int32).at[order].set(r)


def setup_inputs(seed: int = 0, part: int = 0) -> dict:
    ks = jax.random.split(jax.random.fold_in(jax.random.key(seed), part), 8)
    kd = jax.random.split(jax.random.fold_in(jax.random.fold_in(jax.random.key(seed), part), 7), 3)
    kw = jax.random.split(jax.random.key(seed + 1), 5)
    normal_sum = jnp.sum(jax.random.randint(kd[0], (PP, 4, EXPERTS), 0, 256), axis=1)
    octave_step = ((4 * 255 - normal_sum) // 16).astype(jnp.uint32)
    mant_table = jnp.array([256, 279, 304, 332, 362, 395, 431, 470], dtype=jnp.uint32)
    inv_weight = jnp.repeat(mant_table[octave_step & 7] << (octave_step >> 3), M, axis=0)

    def route(i):
        raw_bits = jax.random.bits(jax.random.fold_in(kd[1], i), (T, EXPERTS), jnp.uint32) >> 16
        wait_time = raw_bits * inv_weight[i]
        return jnp.argsort(wait_time, axis=-1)[:, :TOP].astype(jnp.int32)

    idx = lax.map(route, jnp.arange(PP * M))
    n = TD * TOP
    prio = jnp.argsort(jax.random.uniform(kd[2], (PP * M * EP, n)), axis=-1).astype(jnp.int32)
    r = jax.vmap(ranks)(idx.reshape(PP * M * EP, n), prio).reshape(PP * M, EP, TD, TOP)
    first = (jnp.arange(EP, dtype=jnp.int32) * CG)[None, :, None, None]
    slot = jnp.where(r < CG, r + first, -1).reshape(PP, M, SEQS, L, TOP)
    idx = idx.reshape(PP, M, SEQS, L, TOP)
    g = jax.nn.softmax(1.2 * jax.random.normal(ks[2], (PP, M, SEQS, L, TOP)), axis=-1)
    scale = jnp.exp(0.5 * jax.random.normal(ks[3], (PP, 1, EXPERTS, 1, 1)))
    mu = jax.random.normal(ks[4], (PP, 1, EXPERTS, 1, D))
    O = (scale * (jax.random.normal(ks[5], (PP, M, EXPERTS, C, D)) + 0.8 * mu)).astype(jnp.bfloat16)
    H = jax.random.normal(ks[6], (PP, M, SEQS, L, D)).astype(jnp.bfloat16)
    w = 1.0 + 0.4 * jax.random.normal(kw[0], (PP, D))
    sharp = (0.75 * math.log(L)) ** 0.25 / math.sqrt(D)
    Wq = (sharp * jax.random.normal(kw[1], (PP, D, HEADS, HEAD_DIM))).astype(jnp.bfloat16)
    Wk = (sharp * jax.random.normal(kw[2], (PP, D, HEADS, HEAD_DIM))).astype(jnp.bfloat16)
    Wv = (jax.random.normal(kw[3], (PP, D, HEADS, HEAD_DIM)) / math.sqrt(D)).astype(jnp.bfloat16)
    Wo = (jax.random.normal(kw[4], (PP, HEADS, HEAD_DIM, D)) / math.sqrt(QKV)).astype(jnp.bfloat16)
    return dict(O=O, idx=idx, slot=slot, g=g.astype(jnp.float32), H=H, w=w.astype(jnp.float32), Wq=Wq, Wk=Wk, Wv=Wv, Wo=Wo)


def combine(o, ix, sl, gt, h):
    flat = o.reshape(EXPERTS * C, D)
    acc = h.astype(jnp.float32)
    for kk in range(TOP):
        s = sl[:, kk]
        valid = s >= 0
        rows = jnp.take(flat, ix[:, kk] * C + jnp.where(valid, s, 0), axis=0)
        acc = acc + jnp.where(valid, gt[:, kk], 0.0)[:, None] * rows.astype(jnp.float32)
    return acc.astype(jnp.bfloat16)


def head_attn(a):
    qh, kh, vh = a
    s = jnp.dot(qh, kh.T, preferred_element_type=jnp.float32) * (HEAD_DIM ** -0.5)
    r = lax.broadcasted_iota(jnp.int32, (L, L), 0)
    c = lax.broadcasted_iota(jnp.int32, (L, L), 1)
    p = jax.nn.softmax(jnp.where(r >= c, s, -1e30), axis=-1)
    return jnp.dot(p, vh.astype(jnp.float32))


def layer(y, wn, wq, wk, wv, wo):
    yf = y.astype(jnp.float32)
    x = (yf * lax.rsqrt(jnp.mean(yf * yf, axis=-1, keepdims=True) + EPS) * wn).astype(jnp.bfloat16)
    q = jnp.dot(x, wq.reshape(D, QKV), preferred_element_type=jnp.float32).astype(jnp.bfloat16)
    k = jnp.dot(x, wk.reshape(D, QKV), preferred_element_type=jnp.float32).astype(jnp.bfloat16)
    v = jnp.dot(x, wv.reshape(D, QKV), preferred_element_type=jnp.float32).astype(jnp.bfloat16)

    def heads(t):
        return t.reshape(SEQS, L, HEADS, HEAD_DIM).transpose(0, 2, 1, 3).reshape(SEQS * HEADS, L, HEAD_DIM)

    o = lax.map(head_attn, (heads(q), heads(k), heads(v)))
    o = o.reshape(SEQS, HEADS, L, HEAD_DIM).transpose(0, 2, 1, 3).reshape(T, QKV).astype(jnp.bfloat16)
    a = jnp.dot(o, wo.reshape(QKV, D), preferred_element_type=jnp.float32).astype(jnp.bfloat16)
    return (yf + a.astype(jnp.float32)).astype(jnp.bfloat16)


def reference(O, idx, slot, g, H, w, Wq, Wk, Wv, Wo):
    y = lax.map(lambda a: combine(a[0], a[1], a[2], a[3], a[4]),
                (O.reshape(PP * M, EXPERTS, C, D), idx.reshape(PP * M, T, TOP), slot.reshape(PP * M, T, TOP),
                 g.reshape(PP * M, T, TOP), H.reshape(PP * M, T, D)))
    y = jnp.roll(y.reshape(PP, M, T, D), 1, axis=0)

    def stage(a):
        ys, wn, wq, wk, wv, wo = a
        return lax.map(lambda yy: layer(yy, wn, wq, wk, wv, wo), ys)

    z = lax.map(stage, (y, w, Wq, Wk, Wv, Wo))
    return z.reshape(PP, M, SEQS, L, D)
```

```python
import functools
import jax
import jax.numpy as jnp
from jax import lax
from jax.experimental import pallas as pl
from jax.experimental.pallas import tpu as pltpu
from jax.sharding import PartitionSpec as P

EPS = 1e-6
F32, BF16 = jnp.float32, jnp.bfloat16
VMEM_LIMIT = 58 * 1024 * 1024


def params(n):
    return pltpu.CompilerParams(dimension_semantics=("arbitrary",) * n, vmem_limit_bytes=VMEM_LIMIT)


def partial_kernel(cg, nout, has_add, sp, r_ref, o_ref, *rest):
    out_refs, g_ref = rest[-1 - nout:-1], rest[-1]
    ne, _, d = o_ref.shape[1:]
    n, rows = r_ref.shape[2], ne * cg
    q = lax.broadcasted_iota(jnp.int32, (n, rows), 1)
    code = (sp[0] * (ne * cg * 4) + (q // cg) * (cg * 4) + sp[1] * cg + q % cg).astype(F32)
    r = r_ref[0, 0]
    top = r.shape[1] // 2
    gm = jnp.zeros((n, rows), F32)
    for k in range(top):
        gm = jnp.where(r[:, k:k + 1] == code, r[:, top + k:top + k + 1], gm)
    hi = gm.astype(BF16)
    g_ref[0:n] = hi
    r1 = gm - hi.astype(F32)
    mid = r1.astype(BF16)
    g_ref[n:2 * n] = mid
    g_ref[2 * n:] = (r1 - mid.astype(F32)).astype(BF16)
    acc = jnp.dot(g_ref[...], o_ref[0].reshape(rows, d), preferred_element_type=F32)
    s = acc[0:n] + acc[n:2 * n] + acc[2 * n:]
    if has_add:
        s = s + rest[0][0]
    if nout == 1:
        out_refs[0][0] = s
        return
    for i, out_ref in enumerate(out_refs):
        @pl.when(pl.program_id(0) == i)
        def _():
            out_ref[0] = s


def partials(m0, nm, sp, routes, o, add=None, add_at=0, split=False):
    nout = nm if split else 1
    _, ne, cap, d = o.shape
    n, cg = routes.shape[2], cap // 4
    in_specs = [
        pl.BlockSpec((1, 1, n, routes.shape[3]), lambda i, sp: (sp[1], m0 + i, 0, 0)),
        pl.BlockSpec((1, ne, cg, d), lambda i, sp: (m0 + i, 0, sp[1], 0)),
    ]
    ops = [routes, o]
    if add is not None:
        in_specs.append(pl.BlockSpec((1, n, d), lambda i, sp: (add_at + i, 0, 0)))
        ops.append(add)
    return pl.pallas_call(
        functools.partial(partial_kernel, cg, nout, add is not None),
        grid_spec=pltpu.PrefetchScalarGridSpec(
            num_scalar_prefetch=1, grid=(nm,), in_specs=in_specs,
            out_specs=[pl.BlockSpec((1, n, d), lambda i, sp: (0 if split else i, 0, 0))] * nout,
            scratch_shapes=[pltpu.VMEM((3 * n, ne * cg), BF16)]),
        out_shape=[jax.ShapeDtypeStruct((nm // nout, n, d), F32)] * nout,
        compiler_params=params(1), name="partials",
        cost_estimate=pl.CostEstimate(flops=nm * 6 * n * ne * cg * d, transcendentals=0,
                                      bytes_accessed=nm * (ne * cg * d * 2 + n * d * 4)),
    )(sp, *ops)


def relayout_kernel(sp, w_ref, o_ref, s_ref):
    eb, nh = w_ref.shape[1:3]
    for j in range(nh // 8):
        s_ref[...] = w_ref[0, :, j * 8:j * 8 + 8, :].astype(F32).reshape(eb * 8, 128)
        for i in range(8):
            h = j * 8 + i
            o_ref[h // 2, :, (h % 2) * 128:(h % 2) * 128 + 128] = s_ref[pl.ds(i, eb, stride=8), :].astype(BF16)


def relayout(sp, w, eb=512, hb=16):
    _, e, h, f = w.shape
    return pl.pallas_call(
        relayout_kernel,
        grid_spec=pltpu.PrefetchScalarGridSpec(
            num_scalar_prefetch=1, grid=(e // eb, h // 2 // hb),
            in_specs=[pl.BlockSpec((1, eb, hb, f), lambda i, j, sp: (0, i, sp[0] * (h // 2 // hb) + j, 0))],
            out_specs=pl.BlockSpec((hb // 2, eb, 2 * f), lambda i, j, sp: (j, i, 0)),
            scratch_shapes=[pltpu.VMEM((eb * 8, f), F32)]),
        out_shape=jax.ShapeDtypeStruct((h // 4, e, 2 * f), BF16),
        compiler_params=params(2), name="relayout",
        cost_estimate=pl.CostEstimate(flops=10 ** 9, transcendentals=0, bytes_accessed=e * h * f * 2),
    )(sp, w)


def attention(n, qkv, o_refs):
    hd = qkv.shape[1] // 6
    mask = lax.broadcasted_iota(jnp.int32, (n, n), 0) >= lax.broadcasted_iota(jnp.int32, (n, n), 1)
    ones = jnp.ones((n, hd), BF16)
    tiles = [(t, h) for t in range(qkv.shape[0] // n) for h in range(2)]
    part = lambda t, h, j: qkv[t * n:(t + 1) * n, (2 * j + h) * hd:(2 * j + h + 1) * hd]
    ss = [lax.dot_general(part(t, h, 0), part(t, h, 1), (((1,), (1,)), ((), ())), preferred_element_type=F32)
          for t, h in tiles]
    ps = []
    for s in ss:
        s = jnp.where(mask, s * hd ** -0.5, -1e30)
        ps.append(jnp.exp(s - jnp.max(s, axis=-1, keepdims=True)))
    for (t, h), p in zip(tiles, ps):
        hi = p.astype(BF16)
        lo = (p - hi.astype(F32)).astype(BF16)
        ve = jnp.concatenate([part(t, h, 2), ones], axis=1)
        o = jnp.dot(jnp.concatenate([hi, lo], axis=1), jnp.concatenate([ve, ve], axis=0), preferred_element_type=F32)
        nt = o_refs[0].shape[0] // n
        o_refs[t // nt][(t % nt) * n:(t % nt + 1) * n, h * hd:(h + 1) * hd] = (o[:, :hd] / o[:, hd:]).astype(BF16)


def qkva_kernel(n, nu, *refs):
    u_refs, (g_ref, wq_ref, wk_ref, wv_ref, om_ref, os_ref, x_ref, qkv_ref) = refs[:nu], refs[nu:]

    @pl.when(pl.program_id(0) == 0)
    def _():
        at = 0
        for u_ref in u_refs:
            for r in range(0, u_ref.shape[0], 32):
                u = u_ref[r:r + 32].astype(F32)
                x = u * lax.rsqrt(jnp.mean(u * u, axis=-1, keepdims=True) + EPS) * g_ref[...]
                x_ref[at:at + 32] = x.astype(BF16)
                at += 32

    x = x_ref[...]
    f2 = wq_ref.shape[2]
    for j, w_ref in enumerate((wq_ref, wk_ref, wv_ref)):
        qkv_ref[:, j * f2:(j + 1) * f2] = jnp.dot(x, w_ref[0], preferred_element_type=F32).astype(BF16)
    attention(n, qkv_ref[...], (om_ref, os_ref))


def qkva(n, us, gain, wq, wk, wv):
    t = sum(u.shape[0] for u in us)
    d = us[0].shape[1]
    steps, _, f2 = wq.shape
    res = lambda shape: pl.BlockSpec(shape, lambda i: (0, 0), pipeline_mode=pl.Buffered(1))
    wspec = pl.BlockSpec((1, d, f2), lambda i: (i, 0, 0))
    ospec = pl.BlockSpec((t // 2, f2), lambda i: (0, i))
    osh = jax.ShapeDtypeStruct((t // 2, steps * f2), BF16)
    return pl.pallas_call(
        functools.partial(qkva_kernel, n, len(us)), grid=(steps,),
        in_specs=[res(u.shape) for u in us] + [res(gain.shape), wspec, wspec, wspec],
        out_specs=[ospec, ospec], out_shape=[osh, osh],
        scratch_shapes=[pltpu.VMEM((t, d), BF16), pltpu.VMEM((t, 3 * f2), BF16)],
        compiler_params=params(1), name="qkva",
        cost_estimate=pl.CostEstimate(flops=6 * t * d * steps * f2, transcendentals=0,
                                      bytes_accessed=6 * d * steps * f2),
    )(*us, gain, wq, wk, wv)


def oproj_kernel(nu, sp, am_ref, ar_ref, wm_ref, wr_ref, *rest):
    u_refs, z_ref = rest[:nu], rest[-1]
    acc = jnp.dot(am_ref[...], wm_ref[...], preferred_element_type=F32)
    acc = acc + jnp.dot(ar_ref[...], wr_ref[...], preferred_element_type=F32)
    at = 0
    for u_ref in u_refs:
        r = slice(at, at + u_ref.shape[0])
        z_ref[r] = (u_ref[...].astype(F32) + acc[r].astype(BF16).astype(F32)).astype(BF16)
        at += u_ref.shape[0]


def oproj(gi, total, sp, am, ar, wo, us, z, nt=512):
    t, kh = am.shape
    d = wo.shape[1]
    aspec = pl.BlockSpec((t, kh), lambda i, sp: (0, 0), pipeline_mode=pl.Buffered(1))
    in_specs = [aspec, aspec, pl.BlockSpec((kh, nt), lambda i, sp: (sp[0], i)),
                pl.BlockSpec((kh, nt), lambda i, sp: (1 - sp[0], i))]
    in_specs += [pl.BlockSpec((u.shape[0], nt), lambda i, sp: (0, i)) for u in us]
    ops = [sp, am, ar, wo, wo, *us]
    alias = {}
    if z is not None:
        alias = {len(ops): 0}
        in_specs.append(pl.BlockSpec(memory_space=pl.ANY))
        ops.append(z)
    return pl.pallas_call(
        functools.partial(oproj_kernel, len(us)),
        grid_spec=pltpu.PrefetchScalarGridSpec(
            num_scalar_prefetch=1, grid=(d // nt,), in_specs=in_specs,
            out_specs=pl.BlockSpec((t, nt), lambda i, sp: (gi, i))),
        out_shape=jax.ShapeDtypeStruct((total, d), BF16), input_output_aliases=alias,
        compiler_params=params(1), name="oproj",
        cost_estimate=pl.CostEstimate(flops=4 * t * kh * d, transcendentals=0, bytes_accessed=4 * kh * d),
    )(*ops)


def solution(mesh):
    npp, nep = mesh.shape['pp'], mesh.shape['ep']
    yperm = [(i, (i + 1) % npp) for i in range(npp)]
    cperm = [(i, i ^ 1) for i in range(nep)]
    xperm = [(i, i ^ 2) for i in range(nep)]
    tok = P(('data', 'pp'), None, 'ep', None, None)
    wsp = P('pp', None, None, None)

    def body(O, idx, slot, g, H, w, Wq, Wk, Wv, Wo):
        o, h = O[0], H[0, :, 0]
        mb, n, d = h.shape
        cap = o.shape[2]
        ep = lax.axis_index('ep')
        pos = jnp.where(slot[0, :, 0] >= 0, idx[0, :, 0] * cap + slot[0, :, 0], -1).astype(F32)
        routes = lax.all_gather(jnp.concatenate([pos, g[0, :, 0]], axis=-1), 'ep')
        own = [jnp.stack([ep, ep ^ i]).astype(jnp.int32) for i in range(nep)]
        core = (ep % 2).reshape(1).astype(jnp.int32)
        wo = Wo[0].reshape(-1, d)

        last = [own[0]]

        def run(f, sp, *a, **k):
            sp, _ = lax.optimization_barrier((sp, last[0]))
            out = f(sp, *a, **k)
            last[0] = out[0] if isinstance(out, (list, tuple)) else out
            return out

        def part(m0, nm, k, *a, **kw):
            return run(lambda sp: partials(m0, nm, sp, routes, o, *a, **kw), own[k])

        a01 = lax.ppermute(part(0, 2, 3)[0], 'ep', cperm)
        a25 = lax.ppermute(part(2, 4, 3)[0], 'ep', cperm)
        far = part(0, 2, 2, a01, 0, split=True)
        far = [lax.ppermute(f, 'ep', xperm) for f in far]
        rest = part(2, 4, 2, a25, 0, split=True)
        far += [lax.ppermute(f, 'ep', xperm) for f in rest]
        b = lax.ppermute(part(0, mb, 1)[0], 'ep', cperm)

        def rel(W):
            return run(relayout, core, W)

        wq = rel(Wq)
        near = part(0, mb, 0, b, 0)[0]

        def hop(m):
            near_, _ = lax.optimization_barrier((near[m], last[0]))
            y = (h[m].astype(F32) + near_ + far[m][0]).astype(BF16)
            last[0] = y
            u = lax.ppermute(y, 'pp', yperm)
            return u, lax.ppermute(u, 'ep', cperm)

        def attend(us):
            u = [p[0] for p in us] + [p[1] for p in us]
            u[0], _ = lax.optimization_barrier((u[0], last[0]))
            om, os = qkva(n, u, w, wq, wk, wv)
            last[0] = om
            return om, lax.ppermute(os, 'ep', cperm)

        def project(gi, us, am, ar, z):
            return run(lambda sp: oproj(gi, mb * n, sp, am, ar, wo, [p[0] for p in us], z), core)

        u0 = hop(0)
        u1 = hop(1)
        wk = rel(Wk)
        wv = rel(Wv)
        u2 = hop(2)
        at0 = attend([u0, u1])
        u3 = hop(3)
        z = project(0, [u0, u1], *at0, None)
        u4 = hop(4)
        at1 = attend([u2, u3])
        u5 = hop(5)
        z = project(1, [u2, u3], *at1, z)
        at2 = attend([u4, u5])
        z = project(2, [u4, u5], *at2, z)
        return z.reshape(1, mb, 1, n, d)

    return jax.shard_map(body, mesh=mesh,
                         in_specs=(tok, tok, tok, tok, tok, P('pp', None), wsp, wsp, wsp, wsp),
                         out_specs=tok, check_vma=False)
```
